32 devices in a mesh: dp: 8 (over y, x, core), mp: 4 (over z).
Axes of the slice: x: 2, y: 2, z: 4, core: 2. Of those that a mesh axis runs over, the one named last changes fastest.
Arguments:
- tokens: bfloat16 [2048, 6144], P('dp', 'mp'), may hold values from -40 to 40
- norm_gain: float32 [6144], P('mp'), may hold values from 0.1 to 1.9
- w_qkv: bfloat16 [6144, 3, 4096], P('mp', None, 'dp'), may hold values from -0.078125 to 0.078125
- w_up: bfloat16 [6144, 12288], P('mp', 'dp'), may hold values from -0.078125 to 0.078125
- w_attn_out: bfloat16 [4096, 6144], P('dp', 'mp'), may hold values from -0.09375 to 0.09375
- w_down: bfloat16 [12288, 6144], P('dp', 'mp'), may hold values from -0.0546875 to 0.0546875
Outputs:
- layer_out: bfloat16 [2048, 6144], P('dp', 'mp')
The draws below stay inside these ranges and needn't reach their ends.
All inputs are finite; a program needn't handle non-finite values.
Results may differ from the reference program's by a relative error of at most 0.015.
Values may be sent and summed in bfloat16 or wider, within the bound.
A program may use at most 128 MiB of HBM per device.

```python
import jax
import jax.numpy as jnp
from jax import lax

D = 6144
HEADS = 32
HEAD_DIM = 128
FF = 12288
PATCHES = 256
TOKENS = 2048
N_DP = 8
N_MP = 4


def draw_tokens(key, part):
    first = jax.random.fold_in(key, 0)
    ramp = 0.6 * 3.0 ** (jnp.arange(D, dtype=jnp.float32) / D)
    values = jnp.clip(jax.random.normal(first, (TOKENS, D), jnp.float32), -6.0, 6.0) * ramp[None, :]
    return values.astype(jnp.bfloat16)


def levels(own_key, extent, pieces, low, largest):
    level = 1.0
    for dim, blocks in pieces:
        steps = jax.random.uniform(jax.random.fold_in(jax.random.fold_in(own_key, 6), dim), (blocks,), jnp.float32, low / len(pieces), largest / len(pieces))
        level = level * jnp.repeat(jnp.exp(steps), extent[dim] // blocks).reshape((-1,) + (1,) * (len(extent) - 1 - dim))
    return level


def bell_draw(rng, dims, deviation, most, pieces=(), held_as=jnp.bfloat16):
    loudness = levels(rng, dims, pieces, -0.22, 0.18) if pieces else 1.0
    drawn = jax.random.normal(rng, dims, jnp.float32) * deviation * loudness
    return jnp.minimum(jnp.maximum(drawn, -most), most).astype(held_as)


def setup_inputs(seed: int = 0) -> dict:
    splits = jax.random.split(jax.random.key(seed), 7)
    return {
        "tokens": draw_tokens(jax.random.fold_in(splits[6], 71), 0),
        "norm_gain": jnp.clip(1.0 + 0.18 * jax.random.normal(splits[1], (D,), jnp.float32), 0.1, 1.9),
        "w_qkv": bell_draw(splits[2], (D, 3, HEADS * HEAD_DIM), D ** -0.5, 0.078125, ((0, 4), (2, 8))),
        "w_up": bell_draw(splits[3], (D, FF), D ** -0.5, 0.078125, ((0, 4), (1, 8))),
        "w_attn_out": bell_draw(splits[4], (HEADS * HEAD_DIM, D), (HEADS * HEAD_DIM) ** -0.5, 0.09375, ((0, 8), (1, 4))),
        "w_down": bell_draw(splits[5], (FF, D), FF ** -0.5, 0.0546875, ((0, 8), (1, 4))),
    }


EPS = 1e-06

def normalize_rows(values, total, squares, gain, width):
    mean = total / width
    spread = squares / width - mean * mean
    scaled = (values - mean[:, None]) * lax.rsqrt(spread + EPS)[:, None]
    return (scaled * gain[None, :]).astype(jnp.bfloat16)

def head_norm(values):
    mean = lax.optimization_barrier(jnp.mean(values, axis=-1, keepdims=True))
    centered = values - mean
    spread = lax.optimization_barrier(jnp.mean(centered * centered, axis=-1, keepdims=True))
    return centered * lax.rsqrt(spread + EPS)

def attend(qkv, heads_here):
    rows = qkv.shape[0]
    images = rows // PATCHES
    parts = qkv.reshape(images, PATCHES, 3, heads_here, HEAD_DIM)
    query = (head_norm(parts[:, :, 0].astype(jnp.float32)) * (1.0 / HEAD_DIM) ** 0.5).astype(jnp.bfloat16)
    keys = head_norm(parts[:, :, 1].astype(jnp.float32)).astype(jnp.bfloat16)
    values = parts[:, :, 2]
    scores = jnp.einsum('iqhd,ikhd->ihqk', query.astype(jnp.float32), keys.astype(jnp.float32))
    weights = jnp.exp(scores)
    probs = (weights / lax.optimization_barrier(jnp.sum(weights, axis=-1, keepdims=True))).astype(jnp.bfloat16)
    mixed = jnp.einsum('ihqk,ikhd->iqhd', probs.astype(jnp.float32), values.astype(jnp.float32))
    return mixed.astype(jnp.bfloat16).reshape(rows, heads_here * HEAD_DIM)

def reference(tokens, norm_gain, w_qkv, w_up, w_attn_out, w_down):
    xf = tokens.astype(jnp.float32)
    normed = normalize_rows(xf, lax.optimization_barrier(jnp.sum(xf, axis=1)), lax.optimization_barrier(jnp.sum(xf * xf, axis=1)), norm_gain, D)
    head_cols = HEADS * HEAD_DIM
    w_heads = w_qkv.reshape(D, 3 * head_cols)
    feat_block = D // N_MP
    projected = jnp.zeros((TOKENS, 3 * head_cols + FF), jnp.float32)
    for block in range(N_MP):
        first = block * feat_block
        cols = normed[:, first:first + feat_block]
        term = jnp.concatenate([jnp.dot(cols, w_heads[first:first + feat_block], preferred_element_type=jnp.float32), jnp.dot(cols, w_up[first:first + feat_block], preferred_element_type=jnp.float32)], axis=1)
        projected = projected + lax.optimization_barrier(term.astype(jnp.bfloat16)).astype(jnp.float32)
    projected = projected.astype(jnp.bfloat16)
    qkv = projected[:, :3 * head_cols].reshape(TOKENS, 3, head_cols)
    attended = attend(qkv, HEADS)
    activated = jax.nn.gelu(projected[:, 3 * head_cols:].astype(jnp.float32)).astype(jnp.bfloat16)
    head_block = head_cols // N_DP
    unit_block = FF // N_DP
    total = xf
    for block in range(N_DP):
        hfirst = block * head_block
        ufirst = block * unit_block
        term = jnp.dot(attended[:, hfirst:hfirst + head_block], w_attn_out[hfirst:hfirst + head_block], preferred_element_type=jnp.float32)
        term = term + jnp.dot(activated[:, ufirst:ufirst + unit_block], w_down[ufirst:ufirst + unit_block], preferred_element_type=jnp.float32)
        total = total + lax.optimization_barrier(term.astype(jnp.bfloat16)).astype(jnp.float32)
    return total.astype(jnp.bfloat16)
```

```python
import jax
import jax.numpy as jnp
from jax import lax
from jax.sharding import PartitionSpec as P

HEAD_DIM = 128
PATCHES = 256


EPS = 1e-06
UP_SHARES = (1, 2, 2, 1)
FIRST = 1
LAG = 2


def normalize_rows(values, total, squares, gain, width):
    mean = total / width
    spread = squares / width - mean * mean
    scaled = (values - mean[:, None]) * lax.rsqrt(spread + EPS)[:, None]
    return (scaled * gain[None, :]).astype(jnp.bfloat16)


def head_norm(values):
    mean = jnp.mean(values, axis=-1, keepdims=True)
    centered = values - mean
    spread = jnp.mean(centered * centered, axis=-1, keepdims=True)
    return centered * lax.rsqrt(spread + EPS)


def attend(qkv, heads_here):
    rows = qkv.shape[0]
    images = rows // PATCHES
    parts = qkv.reshape(images, PATCHES, 3, heads_here, HEAD_DIM)
    query = (head_norm(parts[:, :, 0].astype(jnp.float32)) * (1.0 / HEAD_DIM) ** 0.5).astype(
        jnp.bfloat16
    )
    keys = head_norm(parts[:, :, 1].astype(jnp.float32)).astype(jnp.bfloat16)
    values = parts[:, :, 2]
    scores = jnp.einsum("iqhd,ikhd->ihqk", query, keys, preferred_element_type=jnp.float32)
    weights = jnp.exp(scores)
    probs = (weights / jnp.sum(weights, axis=-1, keepdims=True)).astype(jnp.bfloat16)
    mixed = jnp.einsum("ihqk,ikhd->iqhd", probs, values, preferred_element_type=jnp.float32)
    return mixed.astype(jnp.bfloat16).reshape(rows, heads_here * HEAD_DIM)


def shift(values, axis, senders, step):
    return lax.ppermute(values, axis, [(i, i + step) for i in senders])


def rows_of(values, block, count):
    return lax.dynamic_slice_in_dim(values, block * count, count, 0)


def add_rounded(*terms):
    total = terms[0].astype(jnp.float32)
    for term in terms[1:]:
        total = total + term.astype(jnp.float32)
    return total.astype(jnp.bfloat16)


class Group:
    def __init__(self, terms, finish, n, me, count):
        self.terms, self.finish, self.n, self.me, self.count = terms, finish, n, me, count
        self.right = self.left = self.own = None
        self.from_left, self.from_right = [], []

    def inputs(self, kind, step):
        n, me, count = self.n, self.me, self.count
        if kind == "scatter":
            send_right = rows_of(self.terms, (me - step - 1) % n, count)
            send_left = rows_of(self.terms, (me + step + 1) % n, count)
            if step:
                send_right = add_rounded(self.right, send_right)
                send_left = add_rounded(self.left, send_left)
            return send_right, send_left
        if step == 0:
            total = add_rounded(rows_of(self.terms, me, count), self.right, self.left)
            self.own = self.finish(total)
            return self.own, self.own
        return self.from_left[-1], self.from_right[-1]

    def move(self, kind, step, send_right, send_left):
        n = self.n
        if kind == "scatter":
            self.right = shift(send_right, "mp", range(step + 1), 1)
            self.left = shift(send_left, "mp", range(n - 1 - step, n), -1)
            return [self.right, self.left]
        self.from_left.append(shift(send_right, "mp", range(step, n - 1), 1))
        self.from_right.append(shift(send_left, "mp", range(1, n - step), -1))
        return [self.from_left[-1], self.from_right[-1]]

    def block(self, r):
        if r == 0:
            return self.own
        near, far = self.from_right[r - 1], self.from_left[self.n - r - 1]
        return jnp.where(self.me + r < self.n, near, far)


def run_line(groups, n):
    if n == 4:
        scatter_at, gather_at, period = [-3, -1, 0], [2, 5, 7], 4
    else:
        scatter_at, gather_at, period = [s - n + 2 for s in range(n - 1)], [2 + s for s in range(n - 1)], n
    slots = {}
    for g, group in enumerate(groups):
        for s in range(n - 1):
            slots.setdefault(g * period + gather_at[s], []).append((group, "gather", s))
            slots.setdefault(g * period + scatter_at[s], []).append((group, "scatter", s))
    history = []
    for at in sorted(slots):
        sends = [pair for group, kind, s in slots[at] for pair in group.inputs(kind, s)]
        if len(history) >= LAG:
            tied = lax.optimization_barrier(tuple(sends) + tuple(history[-LAG]))
            sends = tied[: len(sends)]
        moved = []
        for k, (group, kind, s) in enumerate(slots[at]):
            moved += group.move(kind, s, sends[2 * k], sends[2 * k + 1])
        history.append(moved)


def gather_normed(tokens, stats, n_dp, my_dp, normalize):
    rows, cols = tokens.shape
    if n_dp != 8:
        stats = lax.all_gather(stats, "dp", axis=1, tiled=True)
        return normalize(stats, lax.all_gather(tokens, "dp", axis=0, tiled=True), 0, n_dp)

    def hop(values, offset):
        return lax.ppermute(values, "dp", [(i, i ^ offset) for i in range(n_dp)])

    half = rows // 2
    held = {0: tokens, 2: hop(tokens, 2), 4: hop(tokens, 4)}
    held[1] = hop(tokens, 1)
    stats, held[2], held[4] = lax.optimization_barrier((stats, held[2], held[4]))
    stats = lax.all_gather(stats, "dp", axis=1, tiled=True)
    upper, lower = hop(held[2][:half], 4), hop(held[4][half:], 2)
    held[6] = jnp.concatenate([upper, lower])
    for offset in (2, 4, 6):
        held[offset ^ 1] = hop(held[offset], 1)
    result = jnp.zeros((n_dp * rows, cols), jnp.bfloat16)
    for offset in (0, 1, 2, 3, 4, 5, 6, 7):
        index = my_dp ^ offset
        result = lax.dynamic_update_slice_in_dim(
            result, normalize(stats, held[offset], index, 1), index * rows, 0
        )
    return result


def swap(values, bit, mine, dim, size):
    keep = lax.dynamic_index_in_dim(values, mine, dim, keepdims=False)
    give = lax.dynamic_index_in_dim(values, 1 - mine, dim, keepdims=False)
    got = lax.ppermute(give, "dp", [(i, i ^ (1 << bit)) for i in range(size)])
    return keep, got


def local(tokens, norm_gain, w_qkv, w_up, w_attn_out, w_down):
    n_mp, n_dp = lax.axis_size("mp"), lax.axis_size("dp")
    me, my_dp = lax.axis_index("mp"), lax.axis_index("dp")
    rows_here, feat_here = tokens.shape
    head_cols = w_qkv.shape[2]
    heads_here = head_cols // HEAD_DIM
    units = w_up.shape[1]
    width = feat_here * n_mp
    count = rows_here * n_dp // n_mp
    tokens_f = tokens.astype(jnp.float32)

    stats = lax.psum(
        jnp.stack([jnp.sum(tokens_f, axis=1), jnp.sum(tokens_f * tokens_f, axis=1)]), "mp"
    )

    def normalize(stats, block, index, many):
        here = lax.dynamic_slice_in_dim(stats, index * rows_here, many * rows_here, 1)
        return normalize_rows(block.astype(jnp.float32), here[0], here[1], norm_gain, width)

    normed = gather_normed(tokens, stats, n_dp, my_dp, normalize)

    halves = 2 if heads_here % 2 == 0 else 1
    group_heads = heads_here // halves
    group_cols = group_heads * HEAD_DIM

    def attention(projected):
        return attend(projected.reshape(count, 3, group_cols), group_heads)

    def activation(projected):
        return jax.nn.gelu(projected.astype(jnp.float32)).astype(jnp.bfloat16)

    heads = [("heads", g * group_cols, group_cols) for g in range(halves)]
    ups, first = [], 0
    for share in UP_SHARES:
        ups.append(("up", first, units * share // sum(UP_SHARES)))
        first += units * share // sum(UP_SHARES)
    groups = []
    weights_out = []
    for kind, start, size in ups[:FIRST] + heads + ups[FIRST:]:
        if kind == "heads":
            weight = w_qkv[:, :, start : start + size].reshape(feat_here, 3 * size)
            finish, weight_out = attention, w_attn_out[start : start + size]
        else:
            weight = w_up[:, start : start + size]
            finish, weight_out = activation, w_down[start : start + size]
        terms = jnp.dot(normed, weight, preferred_element_type=jnp.float32).astype(jnp.bfloat16)
        groups.append(Group(terms, finish, n_mp, me, count))
        weights_out.append(weight_out)
    run_line(groups, n_mp)

    order = sorted(range(n_mp), key=lambda r: min(r, n_mp - r))
    out_cols = w_down.shape[1]
    bits = n_dp.bit_length() - 1
    core = my_dp % 2
    pairs = count // rows_here // 2
    kept = jnp.zeros((n_mp * pairs, rows_here, out_cols), jnp.bfloat16)
    for r in order:
        block = sum(
            jnp.dot(group.block(r), weight, preferred_element_type=jnp.float32)
            for group, weight in zip(groups, weights_out)
        ).astype(jnp.bfloat16)
        block = block.reshape(pairs, 2, rows_here, out_cols)
        keep, got = swap(block, 0, core, 1, n_dp)
        kept = lax.dynamic_update_slice_in_dim(
            kept, add_rounded(keep, got), (me + r) % n_mp * pairs, 0
        )
    rest = list(range(1, bits))
    half = out_cols // 2
    results = []
    for part, bit_order in enumerate((rest, rest[::-1])):
        values = kept[:, :, part * half : (part + 1) * half].reshape(
            [2] * len(rest) + [rows_here, half]
        )
        left_bits = list(rest)
        base = tokens_f[:, part * half : (part + 1) * half]
        for bit in bit_order:
            dim = len(left_bits) - 1 - left_bits.index(bit)
            keep, got = swap(values, bit, (my_dp >> bit) % 2, dim, n_dp)
            left_bits.remove(bit)
            if left_bits:
                values = add_rounded(keep, got)
            else:
                total = base + (keep.astype(jnp.float32) + got.astype(jnp.float32))
                results.append(total.astype(jnp.bfloat16))
    return jnp.concatenate(results, axis=1)


def solution(mesh):
    placed = (
        P("dp", "mp"),
        P("mp"),
        P("mp", None, "dp"),
        P("mp", "dp"),
        P("dp", "mp"),
        P("dp", "mp"),
    )
    return jax.shard_map(
        local, mesh=mesh, in_specs=placed, out_specs=P("dp", "mp"), check_vma=False
    )
```
